32 devices in a mesh: gx: 4 (over x, core), gy: 4 (over z), gz: 2 (over y).
Axes of the slice: x: 2, y: 2, z: 4, core: 2. Of those that a mesh axis runs over, the one named last changes fastest.
Arguments:
- deflation: bfloat16 [32, 16, 8, 3, 128], P('gx', 'gy', 'gz'), may hold values from -0.33 to 0.33
- material: int32 [32, 16, 8], P('gx', 'gy', 'gz'), may hold values from 0 to 15
- moduli: float32 [16], replicated, may hold values from 1 to 100
- stencil: float32 [27, 3, 3], replicated, may hold values from -0.6 to 0.6
Outputs:
- coarse: float32 [4, 4, 128, 2, 27, 128], P('gx', 'gy', 'gz')
The draws below stay inside these ranges and needn't reach their ends.
All inputs are finite; a program needn't handle non-finite values.
Results may differ from the reference program's by a relative error of at most 0.005.
Values may be sent and summed in bfloat16 or wider, within the bound.
No kernel may reach another device: no remote copies, remote signals or barrier semaphores. Data moves between devices by JAX's collectives and lax.ppermute only.
A program may use at most 64 MiB of HBM per device.

```python
import math
import jax
import jax.numpy as jnp
from jax import lax

CX = 8
CY = 4
CZ = 4
VECS = 128
NCLASS = 16
NEIGH = 27
NX = 32
NY = 16
NZ = 8
N_GX = 4
N_GY = 4
N_GZ = 2


def draw_deflation(key, part):
    first = jax.random.fold_in(jax.random.fold_in(key, 11), 0)
    shape = (NX, NY, NZ, 3, VECS)
    place_x = jnp.arange(NX, dtype=jnp.int32) % CX
    place_y = jnp.arange(NY, dtype=jnp.int32) % CY
    place_z = jnp.arange(NZ, dtype=jnp.int32) % CZ
    rim_x = jnp.where((place_x == 0) | (place_x == CX - 1), 3.0, 1.0)
    rim_y = jnp.where((place_y == 0) | (place_y == CY - 1), 3.0, 1.0)
    rim_z = jnp.where((place_z == 0) | (place_z == CZ - 1), 3.0, 1.0)
    envelope = rim_x[:, None, None] * rim_y[None, :, None] * rim_z[None, None, :]
    base = jnp.clip(jax.random.normal(first, shape, jnp.float32), -6.0, 6.0)
    return (0.002 * envelope[:, :, :, None, None] * base).astype(jnp.bfloat16)


def place_ends(entries, key, low, largest):
    spot = [jax.random.randint(jax.random.fold_in(key, axis), (), 0, length) for axis, length in enumerate(entries.shape)]
    widest = entries.shape.index(max(entries.shape))
    neighbour = spot[:widest] + [(spot[widest] + 1) % entries.shape[widest]] + spot[widest + 1:]
    return entries.at[tuple(spot)].set(low).at[tuple(neighbour)].set(largest)


def noise(rng, shape, deviation, bound, held_as=jnp.bfloat16):
    array = deviation * jax.random.normal(rng, shape, jnp.float32)
    return jnp.clip(array, min=-bound, max=bound).astype(held_as)


def setup_inputs(seed: int = 0) -> dict:
    keys = jax.random.split(jax.random.key(seed), 5)
    deflation = draw_deflation(jax.random.fold_in(keys[4], 71), 0)
    material = place_ends(jax.random.randint(keys[1], (NX, NY, NZ), 0, NCLASS), jax.random.fold_in(keys[1], 1), 0, NCLASS - 1).astype(jnp.int32)
    moduli = jnp.clip(jnp.exp(jax.random.uniform(keys[2], (NCLASS,), jnp.float32, math.log(1.0), math.log(100.0))), 1.0, 100.0)
    stencil = noise(keys[3], (NEIGH, 3, 3), 0.111, 0.6, jnp.float32)
    return {"deflation": deflation, "material": material, "moduli": moduli, "stencil": stencil}


def offset_list():
    result = []
    for first in (-1, 0, 1):
        for second in (-1, 0, 1):
            for third in (-1, 0, 1):
                result.append((first, second, third))
    return result

def spread(own, stencil):
    len_x = own.shape[0] + 2
    len_y = own.shape[1] + 2
    len_z = own.shape[2] + 2
    padded = jnp.pad(own, ((2, 2), (2, 2), (2, 2), (0, 0), (0, 0))).astype(jnp.float32)
    coupling = stencil.astype(jnp.float32)
    totals = [jnp.zeros((len_x, len_y, len_z, own.shape[4]), jnp.float32) for _ in range(3)]
    for index, offset in enumerate(offset_list()):
        window = padded[1 - offset[0]:1 - offset[0] + len_x, 1 - offset[1]:1 - offset[1] + len_y, 1 - offset[2]:1 - offset[2] + len_z]
        for source in range(3):
            plane = window[:, :, :, source, :]
            for target in range(3):
                totals[target] = totals[target] + coupling[index, source, target] * plane
    return jnp.stack(totals, axis=3)

def region(field, offset):
    pieces = field
    for axis in range(3):
        length = field.shape[axis]
        if offset[axis] < 0:
            start, extent = (0, 1)
        elif offset[axis] == 0:
            start, extent = (1, length - 2)
        else:
            start, extent = (length - 1, 1)
        pieces = lax.slice_in_dim(pieces, start, start + extent, axis=axis)
    return pieces.reshape(-1, pieces.shape[-1])

def contract(left, right):
    return lax.dot_general(left, right, (((0,), (0,)), ((), ())), preferred_element_type=jnp.float32)

def subdomain_blocks(cycle, stencil):
    own = cycle[1:-1, 1:-1, 1:-1]
    image = spread(own, stencil).astype(jnp.bfloat16)
    return jnp.stack([contract(region(image, offset), region(cycle, offset)) for offset in offset_list()])

def reference(deflation, material, moduli, stencil):
    root = jnp.sqrt(moduli)
    cell_roots = root[material]
    padded_vectors = jnp.pad(deflation, ((1, 1), (1, 1), (1, 1), (0, 0), (0, 0)))
    padded_roots = jnp.pad(cell_roots, 1)
    count = N_GX * N_GY * N_GZ

    def single(index):
        first = index // (N_GY * N_GZ)
        second = index // N_GZ % N_GY
        third = index % N_GZ
        block = lax.dynamic_slice(padded_vectors, (first * CX, second * CY, third * CZ, jnp.int32(0), jnp.int32(0)), (CX + 2, CY + 2, CZ + 2, 3, VECS))
        scales = lax.dynamic_slice(padded_roots, (first * CX, second * CY, third * CZ), (CX + 2, CY + 2, CZ + 2))
        cycle = (block.astype(jnp.float32) * scales[:, :, :, None, None]).astype(jnp.bfloat16)
        return subdomain_blocks(cycle, stencil)
    blocks = lax.map(single, jnp.arange(count, dtype=jnp.int32))
    blocks = blocks.reshape(N_GX, N_GY, N_GZ, NEIGH, VECS, VECS)
    return jnp.transpose(blocks, (0, 1, 4, 2, 3, 5))
```

```python
import functools

import jax
import jax.numpy as jnp
from jax import lax
from jax.experimental import pallas as pl
from jax.experimental.pallas import tpu as pltpu
from jax.sharding import PartitionSpec as P

VMEM = pltpu.VMEM
LANES = 128


def scale_kernel(classes, moduli_ref, material_ref, vectors_ref, out_ref):
    cells_y, cells_z, cells_x = material_ref.shape
    parts = vectors_ref.shape[2]
    roots = []
    for y in range(cells_y):
        material = material_ref[y]
        modulus = jnp.zeros(material.shape, jnp.float32)
        for c in range(classes):
            modulus = jnp.where(material == c, moduli_ref[c], modulus)
        roots.append(jnp.sqrt(modulus))
    for x in range(cells_x):
        for y in range(cells_y):
            factor = jnp.broadcast_to(roots[y][:, x : x + 1], (cells_z, vectors_ref.shape[-1]))
            for a in range(parts):
                row = (y * parts + a) * cells_z
                value = vectors_ref[x, y, a].astype(jnp.float32) * factor
                out_ref[x, row : row + cells_z, :] = value.astype(jnp.bfloat16)


def weight_kernel(cells_y, cells_z, table_ref, out_ref):
    count, rows, lanes = out_ref.shape
    half = rows // 2
    table = table_ref[...]
    high = table.astype(jnp.bfloat16)
    low = (table - high.astype(jnp.float32)).astype(jnp.bfloat16)
    row = lax.broadcasted_iota(jnp.int32, (rows, lanes), 0)
    row = jnp.where(row >= half, row - half, row)
    lane = lax.broadcasted_iota(jnp.int32, (rows, lanes), 1)
    block = 3 * cells_z
    row_y, row_z = row // block, row % cells_z
    slot, lane_z = lane // block, lane % cells_z
    lane_y = jnp.where(slot < cells_y, slot, jnp.where(slot == cells_y, -1, cells_y))
    inside = slot < cells_y + 2
    shift_y = lane_y - row_y
    pick_row = lax.broadcasted_iota(jnp.int32, (half, table.shape[0]), 0)
    pick_col = lax.broadcasted_iota(jnp.int32, (half, table.shape[0]), 1)
    part = (pick_row % block) // cells_z
    spread_row = lax.broadcasted_iota(jnp.int32, (table.shape[1], lanes), 0)
    spread_lane = lax.broadcasted_iota(jnp.int32, (table.shape[1], lanes), 1)
    lane_part = (spread_lane % block) // cells_z
    for k in range(3):
        spread = (spread_row == 3 * k + lane_part).astype(jnp.float32).astype(jnp.bfloat16)
        totals = [jnp.zeros((rows, lanes), jnp.float32) for _ in range(3)]
        wide_high = jnp.dot(high, spread, preferred_element_type=jnp.float32).astype(jnp.bfloat16)
        wide_low = jnp.dot(low, spread, preferred_element_type=jnp.float32).astype(jnp.bfloat16)
        for dy in range(3):
            for dz in range(3):
                pick = (pick_col == 9 * part + 3 * dy + dz).astype(jnp.float32).astype(jnp.bfloat16)
                value = jnp.concatenate(
                    [
                        jnp.dot(pick, wide_high, preferred_element_type=jnp.float32),
                        jnp.dot(pick, wide_low, preferred_element_type=jnp.float32),
                    ],
                    axis=0,
                )
                on_y = inside & (shift_y == dy - 1)
                for oz in range(3):
                    shift_z = lane_z + (oz - 1) * cells_z - row_z
                    totals[oz] = jnp.where(on_y & (shift_z == dz - 1), value, totals[oz])
        for oz in range(3):
            out_ref[3 * k + oz] = totals[oz].astype(jnp.bfloat16)


def block_kernel(sizes, weights_ref, field_ref, out_ref, turned_ref, image_ref):
    cells_x, own_rows, rows, owners, share, me = sizes
    width = field_ref.shape[-1]
    first = lax.axis_index("gz") * share
    lane = lax.broadcasted_iota(jnp.int32, (share, LANES), 1)
    side = own_rows // 4
    masks = [
        (lane >= own_rows) & (lane < own_rows + side),
        lane < own_rows,
        (lane >= own_rows + side) & (lane < rows),
    ]
    pad = jnp.zeros((LANES - rows, width), jnp.bfloat16)
    stride = 27 * owners

    def plane(v, x):
        return jnp.concatenate([field_ref[v, x], pad], axis=0)

    for u in range(owners):
        for x in range(cells_x):
            own = field_ref[u, x, 0:own_rows, :]
            turned_ref[...] = jnp.concatenate([own, own], axis=0).T
            image_ref[x * share : (x + 1) * share, :] = turned_ref[pl.ds(first, share), :]
        lhs = image_ref[...]
        for oz in range(3):
            v = u + oz - 1
            if v < 0 or v >= owners:
                zero = jnp.zeros((share, width), jnp.float32)
                for n in range(oz, 27, 3):
                    out_ref[pl.ds(n * owners + u, share, stride=stride), :] = zero
                continue
            products = [
                jnp.dot(lhs, weights_ref[3 * k + oz], preferred_element_type=jnp.float32) for k in range(3)
            ]

            def image(x):
                total = None
                for k in range(3):
                    source = x - (k - 1)
                    if 0 <= source < cells_x:
                        term = products[k][source * share : (source + 1) * share, :]
                        total = term if total is None else total + term
                return jnp.concatenate(
                    [jnp.where(mask, total, 0.0).astype(jnp.bfloat16) for mask in masks], axis=0
                )

            middle = None
            for x in range(0, cells_x, 2):
                left = jnp.concatenate([image(x), image(x + 1)], axis=1)
                right = jnp.concatenate([plane(v, x), plane(v, x + 1)], axis=0)
                term = jnp.dot(left, right, preferred_element_type=jnp.float32)
                middle = term if middle is None else middle + term
            before = jnp.dot(image(-1), plane(v, cells_x), preferred_element_type=jnp.float32)
            after = jnp.dot(image(cells_x), plane(v, cells_x + 1), preferred_element_type=jnp.float32)
            for ox, value in enumerate((before, middle, after)):
                for oy in range(3):
                    n = 9 * ox + 3 * oy + oz
                    out_ref[pl.ds(n * owners + u, share, stride=stride), :] = value[
                        oy * share : (oy + 1) * share, :
                    ]


def cyclic(array, axis, step):
    peers = lax.axis_size(axis)
    return lax.ppermute(array, axis, [(i, (i + step) % peers) for i in range(peers)])


def halo(first, last, axis):
    peers, place = lax.axis_size(axis), lax.axis_index(axis)
    before = cyclic(last, axis, 1)
    after = cyclic(first, axis, -1)
    zero = jnp.zeros_like(before)
    return jnp.where(place == 0, zero, before), jnp.where(place == peers - 1, zero, after)


def body(deflation, material, moduli, stencil):
    cells_x, cells_y, cells_z, parts, width = deflation.shape
    owners = lax.axis_size("gz")
    share = width // owners
    side = parts * cells_z
    own_rows = cells_y * side
    rows = own_rows + 2 * side
    small = pltpu.CompilerParams(vmem_limit_bytes=16 << 20)

    scaled = pl.pallas_call(
        functools.partial(scale_kernel, moduli.shape[0]),
        out_shape=jax.ShapeDtypeStruct((cells_x, own_rows, width), jnp.bfloat16),
        in_specs=[
            pl.BlockSpec(memory_space=pltpu.SMEM),
            pl.BlockSpec(memory_space=VMEM),
            pl.BlockSpec(memory_space=VMEM),
        ],
        out_specs=pl.BlockSpec(memory_space=VMEM),
        compiler_params=small,
        name="scale",
    )(moduli, jnp.transpose(material, (1, 2, 0)), jnp.transpose(deflation, (0, 1, 3, 2, 4)))

    before, after = halo(scaled[:, :side], scaled[:, own_rows - side :], "gy")
    planes = jnp.concatenate([scaled, before, after], axis=1)
    left, right = halo(planes[0:1], planes[cells_x - 1 :], "gx")
    field = jnp.concatenate([planes, left, right], axis=0)
    if owners == 2:
        other = cyclic(field, "gz", 1)
        lines = jnp.where(lax.axis_index("gz") == 0, jnp.stack([field, other]), jnp.stack([other, field]))
    else:
        lines = lax.all_gather(field, "gz")

    table = jnp.transpose(stencil.reshape(3, 9, 3, 3), (2, 1, 0, 3)).reshape(27, 9)
    weights = pl.pallas_call(
        functools.partial(weight_kernel, cells_y, cells_z),
        out_shape=jax.ShapeDtypeStruct((9, 2 * own_rows, LANES), jnp.bfloat16),
        in_specs=[pl.BlockSpec(memory_space=VMEM)],
        out_specs=pl.BlockSpec(memory_space=VMEM),
        compiler_params=small,
        name="weights",
    )(table)

    sizes = (cells_x, own_rows, rows, owners, share, None)
    coarse = pl.pallas_call(
        functools.partial(block_kernel, sizes),
        out_shape=jax.ShapeDtypeStruct((share * 27 * owners, width), jnp.float32),
        in_specs=[pl.BlockSpec(memory_space=VMEM)] * 2,
        out_specs=pl.BlockSpec(memory_space=VMEM),
        scratch_shapes=[
            VMEM((width, 2 * own_rows), jnp.bfloat16),
            VMEM((cells_x * share, 2 * own_rows), jnp.bfloat16),
        ],
        compiler_params=pltpu.CompilerParams(vmem_limit_bytes=32 << 20),
        name="blocks",
    )(weights, lines)
    coarse = coarse.reshape(share, 27, owners, width)
    return jnp.transpose(coarse, (0, 2, 1, 3)).reshape(1, 1, share, owners, 27, width)


def solution(mesh):
    in_specs = (P("gx", "gy", "gz", None, None), P("gx", "gy", "gz"), P(), P())
    out_specs = P("gx", "gy", "gz", None, None, None)
    return jax.shard_map(body, mesh=mesh, in_specs=in_specs, out_specs=out_specs, check_vma=False)
```

```python
import functools

import jax
import jax.numpy as jnp
from jax import lax
from jax.experimental import pallas as pl
from jax.experimental.pallas import tpu as pltpu
from jax.sharding import PartitionSpec as P


VMEM = pltpu.VMEM
LANES = 128


def scale_kernel(moduli_hbm, material_hbm, vectors_hbm, out_ref, moduli_ref, material_ref, vectors_ref, sems):
    copies = [
        pltpu.make_async_copy(source, target, sems.at[i])
        for i, (source, target) in enumerate(
            ((moduli_hbm, moduli_ref), (material_hbm, material_ref), (vectors_hbm, vectors_ref))
        )
    ]
    for copy in copies:
        copy.start()
    copies[0].wait()
    copies[1].wait()
    classes = moduli_ref.shape[0]
    cells_y, cells_z, cells_x = material_ref.shape
    parts = vectors_ref.shape[2]
    roots = []
    for y in range(cells_y):
        material = material_ref[y]
        modulus = jnp.zeros(material.shape, jnp.float32)
        for c in range(classes):
            modulus = jnp.where(material == c, moduli_ref[c], modulus)
        roots.append(jnp.sqrt(modulus))
    copies[2].wait()
    for x in range(cells_x):
        for y in range(cells_y):
            factor = jnp.broadcast_to(roots[y][:, x : x + 1], (cells_z, vectors_ref.shape[-1]))
            for a in range(parts):
                row = (y * parts + a) * cells_z
                value = vectors_ref[x, y, a].astype(jnp.float32) * factor
                out_ref[x, row : row + cells_z, :] = value.astype(jnp.bfloat16)


def weight_kernel(cells_z, stencil_hbm, out_ref, stencil_ref, sem):
    copy = pltpu.make_async_copy(stencil_hbm, stencil_ref, sem)
    copy.start()
    _, rows, lanes = out_ref.shape
    parts, _, neighbours = stencil_ref.shape
    half = rows // 2
    block = parts * cells_z
    cells_y = half // block
    row = lax.broadcasted_iota(jnp.int32, (half, lanes), 0)
    lane = lax.broadcasted_iota(jnp.int32, (half, lanes), 1)
    slot = lane // block
    lane_y = jnp.where(slot < cells_y, slot, jnp.where(slot == cells_y, -1, cells_y))
    shift_y = jnp.where(slot < cells_y + 2, lane_y - row // block, 9)
    shift_z = lane % cells_z - row % cells_z
    pick_row = lax.broadcasted_iota(jnp.int32, (half, parts * neighbours), 0)
    pick_col = lax.broadcasted_iota(jnp.int32, (half, parts * neighbours), 1)
    pick_col = pick_col - neighbours * ((pick_row % block) // cells_z)
    spread = lax.broadcasted_iota(jnp.int32, (parts, lanes), 0) == (
        (lax.broadcasted_iota(jnp.int32, (parts, lanes), 1) % block) // cells_z
    )
    spread = spread.astype(jnp.float32).astype(jnp.bfloat16)
    wide = []
    copy.wait()
    for a in range(parts):
        exact = stencil_ref[a]
        high = exact.astype(jnp.bfloat16)
        low = (exact - high.astype(jnp.float32)).astype(jnp.bfloat16)
        wide.append(
            [
                lax.dot_general(piece, spread, (((0,), (0,)), ((), ())), preferred_element_type=jnp.float32)
                for piece in (high, low)
            ]
        )
    wide = [jnp.concatenate([w[h] for w in wide], axis=0).astype(jnp.bfloat16) for h in range(2)]
    wide = jnp.concatenate(wide, axis=1)
    for k in range(3):
        totals = [[jnp.zeros((half, lanes), jnp.float32) for _ in range(2)] for _ in range(3)]
        for dy in range(3):
            for dz in range(3):
                pick = (pick_col == 9 * k + 3 * dy + dz).astype(jnp.float32).astype(jnp.bfloat16)
                value = jnp.dot(pick, wide, preferred_element_type=jnp.float32)
                for oz in range(3):
                    here = (shift_y == dy - 1) & (shift_z == dz - 1 - (oz - 1) * cells_z)
                    for h in range(2):
                        totals[oz][h] = jnp.where(here, value[:, h * lanes : (h + 1) * lanes], totals[oz][h])
        for oz in range(3):
            for h in range(2):
                out_ref[3 * k + oz, h * half : (h + 1) * half, :] = totals[oz][h].astype(jnp.bfloat16)


def block_kernel(share, places, weights_ref, *refs):
    owners = len(places(0))
    cells, rims, faces = refs[0:owners], refs[owners : 2 * owners], refs[2 * owners : 3 * owners]
    out_ref, turned_ref, image_ref = refs[3 * owners :]
    cells_x, own_rows, width = cells[0].shape
    rim_rows = rims[0].shape[1]
    rows = own_rows + rim_rows
    me = lax.axis_index("gz")
    place = places(me)
    first = me * share
    lane = lax.broadcasted_iota(jnp.int32, (share, LANES), 1)
    masks = [
        (lane >= own_rows) & (lane < own_rows + rim_rows // 2),
        lane < own_rows,
        (lane >= own_rows + rim_rows // 2) & (lane < rows),
    ]
    pad = jnp.zeros((LANES - rows, width), jnp.bfloat16)
    stride = 27 * owners

    def plane(v, x):
        if x < cells_x:
            return jnp.concatenate([cells[v][x], rims[v][x], pad], axis=0)
        return jnp.concatenate([faces[v][x - cells_x], pad], axis=0)

    def put(n, u, value):
        out_ref[pl.ds(n * owners + place[u], share, stride=stride), :] = value

    for u in range(owners):
        for x in range(cells_x):
            own = cells[u][x]
            turned_ref[...] = jnp.concatenate([own, own], axis=0).T
            image_ref[x * share : (x + 1) * share, :] = turned_ref[pl.ds(first, share), :]
        lhs = image_ref[...]
        if owners == 2:
            toward = place[1 - u] - place[u] + 1
            near, missing = [(u, 1), (1 - u, toward)], [2 - toward]
        else:
            near = [(v, v - u + 1) for v in range(max(u - 1, 0), min(u + 2, owners))]
            missing = [oz for oz in range(3) if not 0 <= u + oz - 1 < owners]
        for oz in missing:
            zero = jnp.zeros((share, width), jnp.float32)
            for n in range(0, 27, 3):
                put(n + oz, u, zero)
        for v, oz in near:
            products = [
                jnp.dot(lhs, weights_ref[3 * k + oz], preferred_element_type=jnp.float32) for k in range(3)
            ]

            def image(x):
                total = None
                for k in range(3):
                    source = x - (k - 1)
                    if 0 <= source < cells_x:
                        term = products[k][source * share : (source + 1) * share, :]
                        total = term if total is None else total + term
                return jnp.concatenate(
                    [jnp.where(mask, total, 0.0).astype(jnp.bfloat16) for mask in masks], axis=0
                )

            middle = None
            for x in range(0, cells_x, 2):
                left = jnp.concatenate([image(x), image(x + 1)], axis=1)
                right = jnp.concatenate([plane(v, x), plane(v, x + 1)], axis=0)
                term = jnp.dot(left, right, preferred_element_type=jnp.float32)
                middle = term if middle is None else middle + term
            before = jnp.dot(image(-1), plane(v, cells_x), preferred_element_type=jnp.float32)
            after = jnp.dot(image(cells_x), plane(v, cells_x + 1), preferred_element_type=jnp.float32)
            for ox, value in enumerate((before, middle, after)):
                for oy in range(3):
                    put(9 * ox + 3 * oy + oz, u, value[oy * share : (oy + 1) * share, :])


def in_hbm(array):
    return pltpu.with_memory_space_constraint(array, pltpu.HBM)


def cyclic(array, axis, step):
    peers = lax.axis_size(axis)
    return lax.ppermute(array, axis, [(i, (i + step) % peers) for i in range(peers)])


def halo(first, last, axis):
    peers, place = lax.axis_size(axis), lax.axis_index(axis)
    before = cyclic(last, axis, 1)
    after = cyclic(first, axis, -1)
    zero = jnp.zeros_like(before)
    return jnp.where(place == 0, zero, before), jnp.where(place == peers - 1, zero, after)


def columns(first, last):
    wide, peers = lax.axis_size("gx"), lax.axis_size("gy")
    if wide % 2:
        return halo(first, last, "gy")

    def target(p, q):
        if p % 2 == 0:
            return (p, q + 1) if q + 1 < peers else (p + 1, q)
        return (p, q - 1) if q > 0 else (p - 1, q)

    pairs = []
    for p in range(wide):
        for q in range(peers):
            to_p, to_q = target(p, q)
            pairs.append((p * peers + q, to_p * peers + to_q))
    place = lax.axis_index("gy")
    odd = lax.axis_index("gx") % 2 == 1
    ahead = lax.ppermute(jnp.where(odd, first, last), ("gx", "gy"), pairs)
    back = lax.ppermute(jnp.where(odd, last, first), ("gx", "gy"), [(t, f) for f, t in pairs])
    zero = jnp.zeros_like(ahead)
    before, after = jnp.where(odd, back, ahead), jnp.where(odd, ahead, back)
    return jnp.where(place == 0, zero, before), jnp.where(place == peers - 1, zero, after)


def line(array):
    owners = lax.axis_size("gz")
    if owners == 2:
        return [array, cyclic(array, "gz", 1)]
    gathered = lax.all_gather(array, "gz")
    return [gathered[v] for v in range(owners)]


def blocks(deflation, material, moduli, stencil):
    cells_x, cells_y, cells_z, parts, width = deflation.shape
    owners = lax.axis_size("gz")
    share = width // owners
    side = parts * cells_z
    own_rows = cells_y * side
    small = pltpu.CompilerParams(vmem_limit_bytes=16 << 20)
    vectors = jnp.transpose(deflation, (0, 1, 3, 2, 4))
    classes = jnp.transpose(material, (1, 2, 0))

    scaled = pl.pallas_call(
        scale_kernel,
        out_shape=jax.ShapeDtypeStruct((cells_x, own_rows, width), jnp.bfloat16),
        in_specs=[pl.BlockSpec(memory_space=pltpu.HBM)] * 3,
        out_specs=pl.BlockSpec(memory_space=VMEM),
        scratch_shapes=[
            pltpu.SMEM(moduli.shape, moduli.dtype),
            VMEM(classes.shape, classes.dtype),
            VMEM(vectors.shape, vectors.dtype),
            pltpu.SemaphoreType.DMA((3,)),
        ],
        compiler_params=small,
        name="scale",
    )(*(in_hbm(v) for v in (moduli, classes, vectors)))

    coupling = jnp.transpose(stencil, (1, 2, 0))
    weights = pl.pallas_call(
        functools.partial(weight_kernel, cells_z),
        out_shape=jax.ShapeDtypeStruct((9, 2 * own_rows, LANES), jnp.bfloat16),
        in_specs=[pl.BlockSpec(memory_space=pltpu.HBM)],
        out_specs=pl.BlockSpec(memory_space=VMEM),
        scratch_shapes=[VMEM(coupling.shape, coupling.dtype), pltpu.SemaphoreType.DMA],
        compiler_params=small,
        name="weights",
    )(in_hbm(coupling))

    before, after = columns(scaled[:, :side], scaled[:, own_rows - side :])
    cells = line(scaled)
    rim = jnp.concatenate([before, after], axis=1)
    rims = line(rim)
    first = jnp.concatenate([scaled[0], rim[0]], axis=0)
    last = jnp.concatenate([scaled[cells_x - 1], rim[cells_x - 1]], axis=0)
    left, right = halo(first, last, "gx")
    faces = line(jnp.stack([left, right]))

    def places(me):
        return [me, 1 - me] if owners == 2 else list(range(owners))

    coarse = pl.pallas_call(
        functools.partial(block_kernel, share, places),
        out_shape=jax.ShapeDtypeStruct((share * 27 * owners, width), jnp.float32),
        in_specs=[pl.BlockSpec(memory_space=VMEM)] * (1 + 3 * owners),
        out_specs=pl.BlockSpec(memory_space=VMEM),
        scratch_shapes=[
            VMEM((width, 2 * own_rows), jnp.bfloat16),
            VMEM((cells_x * share, 2 * own_rows), jnp.bfloat16),
        ],
        compiler_params=pltpu.CompilerParams(vmem_limit_bytes=32 << 20),
        name="blocks",
    )(weights, *cells, *rims, *faces)
    coarse = coarse.reshape(share, 27, owners, width)
    return jnp.transpose(coarse, (0, 2, 1, 3)).reshape(1, 1, share, owners, 27, width)


def solution(mesh):
    in_specs = (P("gx", "gy", "gz", None, None), P("gx", "gy", "gz"), P(), P())
    out_specs = P("gx", "gy", "gz", None, None, None)
    return jax.shard_map(blocks, mesh=mesh, in_specs=in_specs, out_specs=out_specs, check_vma=False)
```

```python
import functools

import jax
import jax.numpy as jnp
from jax import lax
from jax.experimental import pallas as pl
from jax.experimental.pallas import tpu as pltpu
from jax.sharding import PartitionSpec as P


VMEM = pltpu.VMEM
LANES = 128


def scale_kernel(
    moduli_hbm, material_hbm, vectors_hbm, stencil_hbm, out_ref, stencil_ref, moduli_ref, material_ref, vectors_ref, sems
):
    copies = [
        pltpu.make_async_copy(source, target, sems.at[i])
        for i, (source, target) in enumerate(
            (
                (moduli_hbm, moduli_ref),
                (material_hbm, material_ref),
                (vectors_hbm, vectors_ref),
                (stencil_hbm, stencil_ref),
            )
        )
    ]
    for copy in copies:
        copy.start()
    copies[0].wait()
    copies[1].wait()
    classes = moduli_ref.shape[0]
    cells_y, cells_z, cells_x = material_ref.shape
    parts = vectors_ref.shape[2]
    roots = []
    for y in range(cells_y):
        material = material_ref[y]
        modulus = jnp.zeros(material.shape, jnp.float32)
        for c in range(classes):
            modulus = jnp.where(material == c, moduli_ref[c], modulus)
        roots.append(jnp.sqrt(modulus))
    copies[2].wait()
    for x in range(cells_x):
        for y in range(cells_y):
            factor = jnp.broadcast_to(roots[y][:, x : x + 1], (cells_z, vectors_ref.shape[-1]))
            for a in range(parts):
                row = (y * parts + a) * cells_z
                value = vectors_ref[x, y, a].astype(jnp.float32) * factor
                out_ref[x, row : row + cells_z, :] = value.astype(jnp.bfloat16)
    copies[3].wait()


def weight_kernel(cells_z, stencil_ref, out_ref):
    _, rows, lanes = out_ref.shape
    parts, _, neighbours = stencil_ref.shape
    half = rows // 2
    block = parts * cells_z
    cells_y = half // block
    row = lax.broadcasted_iota(jnp.int32, (half, lanes), 0)
    lane = lax.broadcasted_iota(jnp.int32, (half, lanes), 1)
    slot = lane // block
    lane_y = jnp.where(slot < cells_y, slot, jnp.where(slot == cells_y, -1, cells_y))
    shift_y = jnp.where(slot < cells_y + 2, lane_y - row // block, 9)
    shift_z = lane % cells_z - row % cells_z
    pick_row = lax.broadcasted_iota(jnp.int32, (half, parts * neighbours), 0)
    pick_col = lax.broadcasted_iota(jnp.int32, (half, parts * neighbours), 1)
    pick_col = pick_col - neighbours * ((pick_row % block) // cells_z)
    spread = lax.broadcasted_iota(jnp.int32, (parts, lanes), 0) == (
        (lax.broadcasted_iota(jnp.int32, (parts, lanes), 1) % block) // cells_z
    )
    spread = spread.astype(jnp.float32).astype(jnp.bfloat16)
    wide = []
    for a in range(parts):
        exact = stencil_ref[a]
        high = exact.astype(jnp.bfloat16)
        low = (exact - high.astype(jnp.float32)).astype(jnp.bfloat16)
        wide.append(
            [
                lax.dot_general(piece, spread, (((0,), (0,)), ((), ())), preferred_element_type=jnp.float32)
                for piece in (high, low)
            ]
        )
    wide = [jnp.concatenate([w[h] for w in wide], axis=0).astype(jnp.bfloat16) for h in range(2)]
    wide = jnp.concatenate(wide, axis=1)
    for k in range(3):
        totals = [[jnp.zeros((half, lanes), jnp.float32) for _ in range(2)] for _ in range(3)]
        for dy in range(3):
            for dz in range(3):
                pick = (pick_col == 9 * k + 3 * dy + dz).astype(jnp.float32).astype(jnp.bfloat16)
                value = jnp.dot(pick, wide, preferred_element_type=jnp.float32)
                for oz in range(3):
                    here = (shift_y == dy - 1) & (shift_z == dz - 1 - (oz - 1) * cells_z)
                    for h in range(2):
                        totals[oz][h] = jnp.where(here, value[:, h * lanes : (h + 1) * lanes], totals[oz][h])
        for oz in range(3):
            for h in range(2):
                out_ref[3 * k + oz, h * half : (h + 1) * half, :] = totals[oz][h].astype(jnp.bfloat16)


def pairs_of(owners, place):
    if owners == 2:
        return [(u, v, place[v] - place[u] + 1) for u in range(2) for v in range(2)]
    return [(u, v, v - u + 1) for u in range(owners) for v in range(max(u - 1, 0), min(u + 2, owners))]


def image_kernel(share, places, rim_rows, weights_ref, *refs):
    owners = len(places(0))
    cells, (out_ref, turned_ref, image_ref) = refs[:owners], refs[owners:]
    cells_x, own_rows, _ = cells[0].shape
    rows = own_rows + rim_rows
    me = lax.axis_index("gz")
    first = me * share
    lane = lax.broadcasted_iota(jnp.int32, (share, LANES), 1)
    masks = [
        (lane >= own_rows) & (lane < own_rows + rim_rows // 2),
        lane < own_rows,
        (lane >= own_rows + rim_rows // 2) & (lane < rows),
    ]
    for u in range(owners):
        for x in range(cells_x):
            own = cells[u][x]
            turned_ref[x] = jnp.concatenate([own, own], axis=0).T
        for x in range(cells_x):
            image_ref[u, x * share : (x + 1) * share, :] = turned_ref[x, pl.ds(first, share), :]
    for pair, (u, v, oz) in enumerate(pairs_of(owners, places(me))):
        lhs = image_ref[u]
        products = [
            jnp.dot(lhs, weights_ref[3 * k + oz], preferred_element_type=jnp.float32) for k in range(3)
        ]
        for slot, x in enumerate([*range(cells_x), -1, cells_x]):
            total = None
            for k in range(3):
                source = x - (k - 1)
                if 0 <= source < cells_x:
                    term = products[k][source * share : (source + 1) * share, :]
                    total = term if total is None else total + term
            for oy, mask in enumerate(masks):
                tile = jnp.where(mask, total, 0.0).astype(jnp.bfloat16)
                out_ref[pair, slot, oy * share : (oy + 1) * share, :] = tile


def filled(pieces):
    pieces = list(pieces)
    missing = LANES - sum(p.shape[0] for p in pieces)
    return jnp.concatenate([*pieces, jnp.zeros((missing, pieces[0].shape[1]), pieces[0].dtype)], axis=0)


def putter(share, owners, out_ref):
    def put(n, u, value):
        out_ref[pl.ds(n * owners + u, share, stride=27 * owners), :] = value

    return put


def sides(share, put, tiles_ref, pair, u, oz, face_ref):
    slot = tiles_ref.shape[1] - 2
    for side in range(2):
        value = jnp.dot(
            tiles_ref[pair, slot + side], filled([face_ref[side]]), preferred_element_type=jnp.float32
        )
        for oy in range(3):
            put(18 * side + 3 * oy + oz, u, value[oy * share : (oy + 1) * share, :])


def middle_kernel(share, places, early, tiles_ref, *refs):
    owners = len(places(0))
    cells, rims, faces, out_ref = refs[:owners], refs[owners : 2 * owners], refs[2 * owners : -1], refs[-1]
    cells_x = cells[0].shape[0]
    place = places(lax.axis_index("gz"))
    put = putter(share, owners, out_ref)
    zero = jnp.zeros((share, out_ref.shape[1]), jnp.float32)
    for u in range(owners):
        if owners == 2:
            lost = [1 - place[1 - u] + place[u]]
        else:
            lost = [oz for oz in range(3) if not 0 <= u + oz - 1 < owners]
        for oz in lost:
            for n in range(0, 27, 3):
                put(n + oz, place[u], zero)
    for pair, (u, v, oz) in enumerate(pairs_of(owners, place)):
        if v in early:
            sides(share, put, tiles_ref, pair, place[u], oz, faces[early.index(v)])
        total = None
        for x in range(0, cells_x, 2):
            left = jnp.concatenate([tiles_ref[pair, x], tiles_ref[pair, x + 1]], axis=1)
            right = jnp.concatenate([filled([cells[v][i], rims[v][i]]) for i in (x, x + 1)], axis=0)
            term = jnp.dot(left, right, preferred_element_type=jnp.float32)
            total = term if total is None else total + term
        for oy in range(3):
            put(9 + 3 * oy + oz, place[u], total[oy * share : (oy + 1) * share, :])


def final_kernel(share, places, late, tiles_ref, *refs):
    faces, (_, whole_ref, out_ref, sem) = refs[: len(late)], refs[len(late) :]
    owners = len(places(0))
    place = places(lax.axis_index("gz"))
    put = putter(share, owners, whole_ref)
    for pair, (u, v, oz) in enumerate(pairs_of(owners, place)):
        if v in late:
            sides(share, put, tiles_ref, pair, place[u], oz, faces[late.index(v)])
    copy = pltpu.make_async_copy(whole_ref, out_ref, sem)
    copy.start()
    copy.wait()


def exchange(array, axes, flips, shift):
    sizes = [lax.axis_size(axis) for axis in axes]
    pairs = []
    for p in range(sizes[0]):
        to_p = (p + 1 if (p - shift) % 2 == 0 else p - 1) % sizes[0]
        if len(axes) == 1:
            pairs.append((p, to_p))
            continue
        for g in range(sizes[1]):
            pairs.append((p * sizes[1] + g, to_p * sizes[1] + (sizes[1] - 1 - g if flips else g)))
    return lax.ppermute(array, axes, pairs)


def sides_of(cells, rims):
    owners, cells_x = len(cells), cells[0].shape[0]
    wide, place = lax.axis_size("gx"), lax.axis_index("gx")

    def edge(v, x):
        return jnp.concatenate([cells[v][x], rims[v][x]], axis=0)

    if wide % 2 or owners != 2:
        left, right = halo(
            jnp.stack([edge(v, 0) for v in range(owners)]),
            jnp.stack([edge(v, cells_x - 1) for v in range(owners)]),
            "gx",
        )
    else:
        odd = place % 2 == 1
        across = jnp.where(odd, edge(0, cells_x - 1), edge(0, 0))
        far = exchange(across, ("gx", "gz"), True, 1)
        next_to = exchange(across, ("gx",), False, 1)
        beside = jnp.stack([jnp.where(odd, edge(v, 0), edge(v, cells_x - 1)) for v in range(owners)])
        beside = exchange(beside, ("gx",), False, 0)
        across = jnp.stack([next_to, far])
        left, right = jnp.where(odd, beside, across), jnp.where(odd, across, beside)
        zero = jnp.zeros_like(left)
        left, right = jnp.where(place == 0, zero, left), jnp.where(place == wide - 1, zero, right)
    return [jnp.stack([left[v], right[v]]) for v in range(owners)]


def in_hbm(array):
    return pltpu.with_memory_space_constraint(array, pltpu.HBM)


def cyclic(array, axis, step):
    peers = lax.axis_size(axis)
    return lax.ppermute(array, axis, [(i, (i + step) % peers) for i in range(peers)])


def halo(first, last, axis):
    peers, place = lax.axis_size(axis), lax.axis_index(axis)
    before = cyclic(last, axis, 1)
    after = cyclic(first, axis, -1)
    zero = jnp.zeros_like(before)
    return jnp.where(place == 0, zero, before), jnp.where(place == peers - 1, zero, after)


def columns(first, last):
    wide, peers = lax.axis_size("gx"), lax.axis_size("gy")
    if wide % 2:
        return halo(first, last, "gy")

    def target(p, q):
        if p % 2 == 0:
            return (p, q + 1) if q + 1 < peers else (p + 1, q)
        return (p, q - 1) if q > 0 else (p - 1, q)

    pairs = []
    for p in range(wide):
        for q in range(peers):
            to_p, to_q = target(p, q)
            pairs.append((p * peers + q, to_p * peers + to_q))
    place = lax.axis_index("gy")
    odd = lax.axis_index("gx") % 2 == 1
    ahead = lax.ppermute(jnp.where(odd, first, last), ("gx", "gy"), pairs)
    back = lax.ppermute(jnp.where(odd, last, first), ("gx", "gy"), [(t, f) for f, t in pairs])
    zero = jnp.zeros_like(ahead)
    before, after = jnp.where(odd, back, ahead), jnp.where(odd, ahead, back)
    return jnp.where(place == 0, zero, before), jnp.where(place == peers - 1, zero, after)


def line(array):
    owners = lax.axis_size("gz")
    if owners == 2:
        return [array, cyclic(array, "gz", 1)]
    gathered = lax.all_gather(array, "gz")
    return [gathered[v] for v in range(owners)]


def blocks(deflation, material, moduli, stencil):
    cells_x, cells_y, cells_z, parts, width = deflation.shape
    owners = lax.axis_size("gz")
    share = width // owners
    side = parts * cells_z
    own_rows = cells_y * side
    small = pltpu.CompilerParams(vmem_limit_bytes=16 << 20)
    vectors = jnp.transpose(deflation, (0, 1, 3, 2, 4))
    classes = jnp.transpose(material, (1, 2, 0))

    coupling = jnp.transpose(stencil, (1, 2, 0))
    scaled, coupling = pl.pallas_call(
        scale_kernel,
        out_shape=(
            jax.ShapeDtypeStruct((cells_x, own_rows, width), jnp.bfloat16),
            jax.ShapeDtypeStruct(coupling.shape, coupling.dtype),
        ),
        in_specs=[pl.BlockSpec(memory_space=pltpu.HBM)] * 4,
        out_specs=(pl.BlockSpec(memory_space=VMEM), pl.BlockSpec(memory_space=VMEM)),
        scratch_shapes=[
            pltpu.SMEM(moduli.shape, moduli.dtype),
            VMEM(classes.shape, classes.dtype),
            VMEM(vectors.shape, vectors.dtype),
            pltpu.SemaphoreType.DMA((4,)),
        ],
        compiler_params=small,
        name="scale",
    )(*(in_hbm(v) for v in (moduli, classes, vectors, coupling)))

    weights = pl.pallas_call(
        functools.partial(weight_kernel, cells_z),
        out_shape=jax.ShapeDtypeStruct((9, 2 * own_rows, LANES), jnp.bfloat16),
        in_specs=[pl.BlockSpec(memory_space=VMEM)],
        out_specs=pl.BlockSpec(memory_space=VMEM),
        compiler_params=small,
        name="weights",
    )(coupling)

    before, after = columns(scaled[:, :side], scaled[:, own_rows - side :])
    cells = line(scaled)
    rim = jnp.concatenate([before, after], axis=1)
    rims = line(rim)
    faces = sides_of(cells, rims)

    def places(me):
        return [me, 1 - me] if owners == 2 else list(range(owners))

    count = len(pairs_of(owners, places(0)))
    early = []
    late = [v for v in range(owners) if v not in early]
    in_vmem = pl.BlockSpec(memory_space=VMEM)
    tiles = pl.pallas_call(
        functools.partial(image_kernel, share, places, 2 * side),
        out_shape=jax.ShapeDtypeStruct((count, cells_x + 2, 3 * share, LANES), jnp.bfloat16),
        in_specs=[in_vmem] * (1 + owners),
        out_specs=in_vmem,
        scratch_shapes=[
            VMEM((cells_x, width, 2 * own_rows), jnp.bfloat16),
            VMEM((owners, cells_x * share, 2 * own_rows), jnp.bfloat16),
        ],
        compiler_params=small,
        name="image",
    )(weights, *cells)
    whole = jax.ShapeDtypeStruct((share * 27 * owners, width), jnp.float32)
    coarse = pl.pallas_call(
        functools.partial(middle_kernel, share, places, early),
        out_shape=pltpu.VMEM(whole.shape, whole.dtype),
        in_specs=[in_vmem] * (1 + 2 * owners + len(early)),
        out_specs=in_vmem,
        compiler_params=small,
        name="middle",
    )(tiles, *cells, *rims, *(faces[v] for v in early))
    _, coarse = pl.pallas_call(
        functools.partial(final_kernel, share, places, late),
        out_shape=(pltpu.VMEM(whole.shape, whole.dtype), whole),
        in_specs=[in_vmem] * (2 + len(late)),
        out_specs=(in_vmem, pl.BlockSpec(memory_space=pltpu.HBM)),
        scratch_shapes=[pltpu.SemaphoreType.DMA],
        input_output_aliases={1 + len(late): 0},
        compiler_params=small,
        name="final",
    )(tiles, *(faces[v] for v in late), coarse)
    coarse = coarse.reshape(share, 27, owners, width)
    return jnp.transpose(coarse, (0, 2, 1, 3)).reshape(1, 1, share, owners, 27, width)


def solution(mesh):
    in_specs = (P("gx", "gy", "gz", None, None), P("gx", "gy", "gz"), P(), P())
    out_specs = P("gx", "gy", "gz", None, None, None)
    return jax.shard_map(blocks, mesh=mesh, in_specs=in_specs, out_specs=out_specs, check_vma=False)
```

```python
import functools

import jax
import jax.numpy as jnp
from jax import lax
from jax.experimental import pallas as pl
from jax.experimental.pallas import tpu as pltpu
from jax.sharding import PartitionSpec as P


VMEM = pltpu.VMEM
LANES = 128
ROUNDS = 2
PIECES = 4


def scale_kernel(
    moduli_hbm, material_hbm, vectors_hbm, stencil_hbm, out_ref, stencil_ref, moduli_ref, material_ref, vectors_ref, sems
):
    copies = [
        pltpu.make_async_copy(source, target, sems.at[i])
        for i, (source, target) in enumerate(
            (
                (moduli_hbm, moduli_ref),
                (material_hbm, material_ref),
                (stencil_hbm, stencil_ref),
            )
        )
    ]
    parts_x = vectors_ref.shape[0] // PIECES
    pieces = [pl.ds(i * parts_x, parts_x) for i in range(PIECES)]
    copies[2:2] = [
        pltpu.make_async_copy(vectors_hbm.at[piece], vectors_ref.at[piece], sems.at[3 + i])
        for i, piece in enumerate(pieces)
    ]
    for copy in copies:
        copy.start()
    copies[0].wait()
    copies[1].wait()
    classes = moduli_ref.shape[0]
    cells_y, cells_z, cells_x = material_ref.shape
    parts = vectors_ref.shape[2]
    roots = []
    for y in range(cells_y):
        material = material_ref[y]
        modulus = jnp.zeros(material.shape, jnp.float32)
        for c in range(classes):
            modulus = jnp.where(material == c, moduli_ref[c], modulus)
        roots.append(jnp.sqrt(modulus))
    for copy in copies[2:-1]:
        copy.wait()
    for x in range(cells_x):
        for y in range(cells_y):
            factor = jnp.broadcast_to(roots[y][:, x : x + 1], (cells_z, vectors_ref.shape[-1]))
            for a in range(parts):
                row = (y * parts + a) * cells_z
                value = vectors_ref[x, y, a].astype(jnp.float32) * factor
                out_ref[x, row : row + cells_z, :] = value.astype(jnp.bfloat16)
    copies[-1].wait()


def weight_kernel(cells_z, stencil_ref, out_ref):
    _, rows, lanes = out_ref.shape
    parts, _, neighbours = stencil_ref.shape
    half = rows // 2
    block = parts * cells_z
    cells_y = half // block
    row = lax.broadcasted_iota(jnp.int32, (half, lanes), 0)
    lane = lax.broadcasted_iota(jnp.int32, (half, lanes), 1)
    slot = lane // block
    lane_y = jnp.where(slot < cells_y, slot, jnp.where(slot == cells_y, -1, cells_y))
    shift_y = jnp.where(slot < cells_y + 2, lane_y - row // block, 9)
    shift_z = lane % cells_z - row % cells_z
    pick_row = lax.broadcasted_iota(jnp.int32, (half, parts * neighbours), 0)
    pick_col = lax.broadcasted_iota(jnp.int32, (half, parts * neighbours), 1)
    pick_col = pick_col - neighbours * ((pick_row % block) // cells_z)
    spread = lax.broadcasted_iota(jnp.int32, (parts, lanes), 0) == (
        (lax.broadcasted_iota(jnp.int32, (parts, lanes), 1) % block) // cells_z
    )
    spread = spread.astype(jnp.float32).astype(jnp.bfloat16)
    wide = []
    for a in range(parts):
        exact = stencil_ref[a]
        high = exact.astype(jnp.bfloat16)
        low = (exact - high.astype(jnp.float32)).astype(jnp.bfloat16)
        wide.append(
            [
                lax.dot_general(piece, spread, (((0,), (0,)), ((), ())), preferred_element_type=jnp.float32)
                for piece in (high, low)
            ]
        )
    wide = [jnp.concatenate([w[h] for w in wide], axis=0).astype(jnp.bfloat16) for h in range(2)]
    wide = jnp.concatenate(wide, axis=1)
    for k in range(3):
        totals = [[jnp.zeros((half, lanes), jnp.float32) for _ in range(2)] for _ in range(3)]
        for dy in range(3):
            for dz in range(3):
                pick = (pick_col == 9 * k + 3 * dy + dz).astype(jnp.float32).astype(jnp.bfloat16)
                value = jnp.dot(pick, wide, preferred_element_type=jnp.float32)
                for oz in range(3):
                    here = (shift_y == dy - 1) & (shift_z == dz - 1 - (oz - 1) * cells_z)
                    for h in range(2):
                        totals[oz][h] = jnp.where(here, value[:, h * lanes : (h + 1) * lanes], totals[oz][h])
        for oz in range(3):
            for h in range(2):
                out_ref[3 * k + oz, h * half : (h + 1) * half, :] = totals[oz][h].astype(jnp.bfloat16)


def pairs_of(owners, place):
    if owners == 2:
        return [(u, v, place[v] - place[u] + 1) for u in range(2) for v in range(2)]
    return [(u, v, v - u + 1) for u in range(owners) for v in range(max(u - 1, 0), min(u + 2, owners))]


def image_kernel(share, places, rim_rows, weights_ref, *refs):
    owners = len(places(0))
    cells, (out_ref, turned_ref, image_ref) = refs[:owners], refs[owners:]
    cells_x, own_rows, _ = cells[0].shape
    rows = own_rows + rim_rows
    me = lax.axis_index("gz")
    first = me * share
    lane = lax.broadcasted_iota(jnp.int32, (share, LANES), 1)
    masks = [
        (lane >= own_rows) & (lane < own_rows + rim_rows // 2),
        lane < own_rows,
        (lane >= own_rows + rim_rows // 2) & (lane < rows),
    ]
    for u in range(owners):
        for x in range(cells_x):
            own = cells[u][x]
            turned_ref[x] = jnp.concatenate([own, own], axis=0).T
        for x in range(cells_x):
            image_ref[u, x * share : (x + 1) * share, :] = turned_ref[x, pl.ds(first, share), :]
    for pair, (u, v, oz) in enumerate(pairs_of(owners, places(me))):
        lhs = image_ref[u]
        products = [
            jnp.dot(lhs, weights_ref[3 * k + oz], preferred_element_type=jnp.float32) for k in range(3)
        ]
        for slot, x in enumerate([*range(cells_x), -1, cells_x]):
            total = None
            for k in range(3):
                source = x - (k - 1)
                if 0 <= source < cells_x:
                    term = products[k][source * share : (source + 1) * share, :]
                    total = term if total is None else total + term
            for oy, mask in enumerate(masks):
                tile = jnp.where(mask, total, 0.0).astype(jnp.bfloat16)
                out_ref[pair, slot, oy * share : (oy + 1) * share, :] = tile


def filled(pieces):
    pieces = list(pieces)
    missing = LANES - sum(p.shape[0] for p in pieces)
    return jnp.concatenate([*pieces, jnp.zeros((missing, pieces[0].shape[1]), pieces[0].dtype)], axis=0)


def putter(share, owners, out_ref, start=0):
    def put(n, u, value):
        out_ref[pl.ds((start * 27 + n) * owners + u, share, stride=27 * owners), :] = value

    return put


def sides(share, put, tiles_ref, pair, u, oz, face_ref, start, size):
    slot = tiles_ref.shape[1] - 2
    for side in range(2):
        left = jnp.concatenate(
            [tiles_ref[pair, slot + side, oy * share + start : oy * share + start + size, :] for oy in range(3)],
            axis=0,
        )
        value = jnp.dot(left, filled([face_ref[side]]), preferred_element_type=jnp.float32)
        for oy in range(3):
            put(18 * side + 3 * oy + oz, u, value[oy * size : (oy + 1) * size, :])


def middle_kernel(share, places, tiles_ref, *refs):
    owners = len(places(0))
    cells, rims, out_ref = refs[:owners], refs[owners : 2 * owners], refs[-1]
    cells_x = cells[0].shape[0]
    place = places(lax.axis_index("gz"))
    put = putter(share, owners, out_ref)
    zero = jnp.zeros((share, out_ref.shape[1]), jnp.float32)
    for u in range(owners):
        if owners == 2:
            lost = [1 - place[1 - u] + place[u]]
        else:
            lost = [oz for oz in range(3) if not 0 <= u + oz - 1 < owners]
        for oz in lost:
            for n in range(0, 27, 3):
                put(n + oz, place[u], zero)
    for pair, (u, v, oz) in enumerate(pairs_of(owners, place)):
        total = None
        for x in range(0, cells_x, 2):
            left = jnp.concatenate([tiles_ref[pair, x], tiles_ref[pair, x + 1]], axis=1)
            right = jnp.concatenate([filled([cells[v][i], rims[v][i]]) for i in (x, x + 1)], axis=0)
            term = jnp.dot(left, right, preferred_element_type=jnp.float32)
            total = term if total is None else total + term
        for oy in range(3):
            put(9 + 3 * oy + oz, place[u], total[oy * share : (oy + 1) * share, :])


def final_kernel(share, places, late, tiles_ref, *refs):
    faces, (_, whole_ref, out_ref, sem) = refs[: len(late)], refs[len(late) :]
    owners = len(places(0))
    place = places(lax.axis_index("gz"))
    rounds = sem.shape[0]
    size = share // rounds
    copies = []
    for i in range(rounds):
        put = putter(size, owners, whole_ref, i * size)
        for pair, (u, v, oz) in enumerate(pairs_of(owners, place)):
            sides(share, put, tiles_ref, pair, place[u], oz, faces[late.index(v)], i * size, size)
        span = pl.ds(i * size * 27 * owners, size * 27 * owners)
        copies.append(pltpu.make_async_copy(whole_ref.at[span], out_ref.at[span], sem.at[i]))
        copies[-1].start()
    for copy in copies:
        copy.wait()


def exchange(array, axes, flips, shift):
    sizes = [lax.axis_size(axis) for axis in axes]
    pairs = []
    for p in range(sizes[0]):
        to_p = (p + 1 if (p - shift) % 2 == 0 else p - 1) % sizes[0]
        if len(axes) == 1:
            pairs.append((p, to_p))
            continue
        for g in range(sizes[1]):
            pairs.append((p * sizes[1] + g, to_p * sizes[1] + (sizes[1] - 1 - g if flips else g)))
    return lax.ppermute(array, axes, pairs)


def sides_of(cells, rims):
    owners, cells_x = len(cells), cells[0].shape[0]
    wide, place = lax.axis_size("gx"), lax.axis_index("gx")

    def edge(v, x):
        return jnp.concatenate([cells[v][x], rims[v][x]], axis=0)

    if wide % 2 or owners != 2:
        left, right = halo(
            jnp.stack([edge(v, 0) for v in range(owners)]),
            jnp.stack([edge(v, cells_x - 1) for v in range(owners)]),
            "gx",
        )
    else:
        odd = place % 2 == 1
        across = jnp.where(odd, edge(0, cells_x - 1), edge(0, 0))
        far = exchange(across, ("gx", "gz"), True, 1)
        next_to = exchange(across, ("gx",), False, 1)
        beside = jnp.stack([jnp.where(odd, edge(v, 0), edge(v, cells_x - 1)) for v in range(owners)])
        beside = exchange(beside, ("gx",), False, 0)
        across = jnp.stack([next_to, far])
        left, right = jnp.where(odd, beside, across), jnp.where(odd, across, beside)
        zero = jnp.zeros_like(left)
        left, right = jnp.where(place == 0, zero, left), jnp.where(place == wide - 1, zero, right)
    return [jnp.stack([left[v], right[v]]) for v in range(owners)]


def in_hbm(array):
    return pltpu.with_memory_space_constraint(array, pltpu.HBM)


def cyclic(array, axis, step):
    peers = lax.axis_size(axis)
    return lax.ppermute(array, axis, [(i, (i + step) % peers) for i in range(peers)])


def halo(first, last, axis):
    peers, place = lax.axis_size(axis), lax.axis_index(axis)
    before = cyclic(last, axis, 1)
    after = cyclic(first, axis, -1)
    zero = jnp.zeros_like(before)
    return jnp.where(place == 0, zero, before), jnp.where(place == peers - 1, zero, after)


def columns(first, last):
    wide, peers = lax.axis_size("gx"), lax.axis_size("gy")
    if wide % 2:
        return halo(first, last, "gy")

    def target(p, q):
        if p % 2 == 0:
            return (p, q + 1) if q + 1 < peers else (p + 1, q)
        return (p, q - 1) if q > 0 else (p - 1, q)

    pairs = []
    for p in range(wide):
        for q in range(peers):
            to_p, to_q = target(p, q)
            pairs.append((p * peers + q, to_p * peers + to_q))
    place = lax.axis_index("gy")
    odd = lax.axis_index("gx") % 2 == 1
    ahead = lax.ppermute(jnp.where(odd, first, last), ("gx", "gy"), pairs)
    back = lax.ppermute(jnp.where(odd, last, first), ("gx", "gy"), [(t, f) for f, t in pairs])
    zero = jnp.zeros_like(ahead)
    before, after = jnp.where(odd, back, ahead), jnp.where(odd, ahead, back)
    return jnp.where(place == 0, zero, before), jnp.where(place == peers - 1, zero, after)


def line(array):
    owners = lax.axis_size("gz")
    if owners == 2:
        return [array, cyclic(array, "gz", 1)]
    gathered = lax.all_gather(array, "gz")
    return [gathered[v] for v in range(owners)]


def blocks(deflation, material, moduli, stencil):
    cells_x, cells_y, cells_z, parts, width = deflation.shape
    owners = lax.axis_size("gz")
    share = width // owners
    side = parts * cells_z
    own_rows = cells_y * side
    small = pltpu.CompilerParams(vmem_limit_bytes=16 << 20)
    vectors = jnp.transpose(deflation, (0, 1, 3, 2, 4))
    classes = jnp.transpose(material, (1, 2, 0))

    coupling = jnp.transpose(stencil, (1, 2, 0))
    scaled, coupling = pl.pallas_call(
        scale_kernel,
        out_shape=(
            jax.ShapeDtypeStruct((cells_x, own_rows, width), jnp.bfloat16),
            jax.ShapeDtypeStruct(coupling.shape, coupling.dtype),
        ),
        in_specs=[pl.BlockSpec(memory_space=pltpu.HBM)] * 4,
        out_specs=(pl.BlockSpec(memory_space=VMEM), pl.BlockSpec(memory_space=VMEM)),
        scratch_shapes=[
            pltpu.SMEM(moduli.shape, moduli.dtype),
            VMEM(classes.shape, classes.dtype),
            VMEM(vectors.shape, vectors.dtype),
            pltpu.SemaphoreType.DMA((3 + PIECES,)),
        ],
        compiler_params=small,
        name="scale",
    )(*(in_hbm(v) for v in (moduli, classes, vectors, coupling)))

    weights = pl.pallas_call(
        functools.partial(weight_kernel, cells_z),
        out_shape=jax.ShapeDtypeStruct((9, 2 * own_rows, LANES), jnp.bfloat16),
        in_specs=[pl.BlockSpec(memory_space=VMEM)],
        out_specs=pl.BlockSpec(memory_space=VMEM),
        compiler_params=small,
        name="weights",
    )(coupling)

    before, after = columns(scaled[:, :side], scaled[:, own_rows - side :])
    cells = line(scaled)
    rim = jnp.concatenate([before, after], axis=1)
    rims = line(rim)
    faces = sides_of(cells, rims)

    def places(me):
        return [me, 1 - me] if owners == 2 else list(range(owners))

    count = len(pairs_of(owners, places(0)))
    early = []
    late = [v for v in range(owners) if v not in early]
    in_vmem = pl.BlockSpec(memory_space=VMEM)
    tiles = pl.pallas_call(
        functools.partial(image_kernel, share, places, 2 * side),
        out_shape=jax.ShapeDtypeStruct((count, cells_x + 2, 3 * share, LANES), jnp.bfloat16),
        in_specs=[in_vmem] * (1 + owners),
        out_specs=in_vmem,
        scratch_shapes=[
            VMEM((cells_x, width, 2 * own_rows), jnp.bfloat16),
            VMEM((owners, cells_x * share, 2 * own_rows), jnp.bfloat16),
        ],
        compiler_params=small,
        name="image",
    )(weights, *cells)
    whole = jax.ShapeDtypeStruct((share * 27 * owners, width), jnp.float32)
    coarse = pl.pallas_call(
        functools.partial(middle_kernel, share, places),
        out_shape=pltpu.VMEM(whole.shape, whole.dtype),
        in_specs=[in_vmem] * (1 + 2 * owners + len(early)),
        out_specs=in_vmem,
        compiler_params=small,
        name="middle",
    )(tiles, *cells, *rims, *(faces[v] for v in early))
    _, coarse = pl.pallas_call(
        functools.partial(final_kernel, share, places, late),
        out_shape=(pltpu.VMEM(whole.shape, whole.dtype), whole),
        in_specs=[in_vmem] * (2 + len(late)),
        out_specs=(in_vmem, pl.BlockSpec(memory_space=pltpu.HBM)),
        scratch_shapes=[pltpu.SemaphoreType.DMA((ROUNDS,))],
        input_output_aliases={1 + len(late): 0},
        compiler_params=small,
        name="final",
    )(tiles, *(faces[v] for v in late), coarse)
    coarse = coarse.reshape(share, 27, owners, width)
    return jnp.transpose(coarse, (0, 2, 1, 3)).reshape(1, 1, share, owners, 27, width)


def solution(mesh):
    in_specs = (P("gx", "gy", "gz", None, None), P("gx", "gy", "gz"), P(), P())
    out_specs = P("gx", "gy", "gz", None, None, None)
    return jax.shard_map(blocks, mesh=mesh, in_specs=in_specs, out_specs=out_specs, check_vma=False)
```

```python
import functools

import jax
import jax.numpy as jnp
from jax import lax
from jax.experimental import pallas as pl
from jax.experimental.pallas import tpu as pltpu
from jax.sharding import PartitionSpec as P


VMEM = pltpu.VMEM
LANES = 128
ROUNDS = 2
PIECES = 4


def scale_kernel(
    moduli_hbm, material_hbm, vectors_hbm, stencil_hbm, out_ref, stencil_ref, moduli_ref, material_ref, vectors_ref, sems
):
    copies = [
        pltpu.make_async_copy(source, target, sems.at[i])
        for i, (source, target) in enumerate(
            (
                (moduli_hbm, moduli_ref),
                (material_hbm, material_ref),
                (stencil_hbm, stencil_ref),
            )
        )
    ]
    parts_x = vectors_ref.shape[0] // PIECES
    pieces = [pl.ds(i * parts_x, parts_x) for i in range(PIECES)]
    copies[2:2] = [
        pltpu.make_async_copy(vectors_hbm.at[piece], vectors_ref.at[piece], sems.at[3 + i])
        for i, piece in enumerate(pieces)
    ]
    for copy in copies:
        copy.start()
    copies[0].wait()
    copies[1].wait()
    classes = moduli_ref.shape[0]
    cells_y, cells_z, cells_x = material_ref.shape
    parts = vectors_ref.shape[2]
    roots = []
    for y in range(cells_y):
        material = material_ref[y]
        modulus = jnp.zeros(material.shape, jnp.float32)
        for c in range(classes):
            modulus = jnp.where(material == c, moduli_ref[c], modulus)
        roots.append(jnp.sqrt(modulus))
    for copy in copies[2:-1]:
        copy.wait()
    for x in range(cells_x):
        for y in range(cells_y):
            factor = jnp.broadcast_to(roots[y][:, x : x + 1], (cells_z, vectors_ref.shape[-1]))
            for a in range(parts):
                row = (y * parts + a) * cells_z
                value = vectors_ref[x, y, a].astype(jnp.float32) * factor
                out_ref[x, row : row + cells_z, :] = value.astype(jnp.bfloat16)
    copies[-1].wait()


def weight_kernel(cells_z, stencil_ref, out_ref):
    _, rows, lanes = out_ref.shape
    parts, _, neighbours = stencil_ref.shape
    half = rows // 2
    block = parts * cells_z
    cells_y = half // block
    row = lax.broadcasted_iota(jnp.int32, (half, lanes), 0)
    lane = lax.broadcasted_iota(jnp.int32, (half, lanes), 1)
    slot = lane // block
    lane_y = jnp.where(slot < cells_y, slot, jnp.where(slot == cells_y, -1, cells_y))
    shift_y = jnp.where(slot < cells_y + 2, lane_y - row // block, 9)
    shift_z = lane % cells_z - row % cells_z
    pick_row = lax.broadcasted_iota(jnp.int32, (half, parts * neighbours), 0)
    pick_col = lax.broadcasted_iota(jnp.int32, (half, parts * neighbours), 1)
    pick_col = pick_col - neighbours * ((pick_row % block) // cells_z)
    spread = lax.broadcasted_iota(jnp.int32, (parts, lanes), 0) == (
        (lax.broadcasted_iota(jnp.int32, (parts, lanes), 1) % block) // cells_z
    )
    spread = spread.astype(jnp.float32).astype(jnp.bfloat16)
    wide = []
    for a in range(parts):
        exact = stencil_ref[a]
        high = exact.astype(jnp.bfloat16)
        low = (exact - high.astype(jnp.float32)).astype(jnp.bfloat16)
        wide.append(
            [
                lax.dot_general(piece, spread, (((0,), (0,)), ((), ())), preferred_element_type=jnp.float32)
                for piece in (high, low)
            ]
        )
    wide = [jnp.concatenate([w[h] for w in wide], axis=0).astype(jnp.bfloat16) for h in range(2)]
    wide = jnp.concatenate(wide, axis=1)
    for k in range(3):
        totals = [[jnp.zeros((half, lanes), jnp.float32) for _ in range(2)] for _ in range(3)]
        for dy in range(3):
            for dz in range(3):
                pick = (pick_col == 9 * k + 3 * dy + dz).astype(jnp.float32).astype(jnp.bfloat16)
                value = jnp.dot(pick, wide, preferred_element_type=jnp.float32)
                for oz in range(3):
                    here = (shift_y == dy - 1) & (shift_z == dz - 1 - (oz - 1) * cells_z)
                    for h in range(2):
                        totals[oz][h] = jnp.where(here, value[:, h * lanes : (h + 1) * lanes], totals[oz][h])
        for oz in range(3):
            for h in range(2):
                out_ref[3 * k + oz, h * half : (h + 1) * half, :] = totals[oz][h].astype(jnp.bfloat16)


def pairs_of(owners, place):
    if owners == 2:
        return [(u, v, place[v] - place[u] + 1) for u in range(2) for v in range(2)]
    return [(u, v, v - u + 1) for u in range(owners) for v in range(max(u - 1, 0), min(u + 2, owners))]


def image_kernel(share, places, rim_rows, weights_ref, *refs):
    owners = len(places(0))
    cells, (out_ref, turned_ref, image_ref) = refs[:owners], refs[owners:]
    cells_x, own_rows, _ = cells[0].shape
    rows = own_rows + rim_rows
    me = lax.axis_index("gz")
    first = me * share
    lane = lax.broadcasted_iota(jnp.int32, (share, LANES), 1)
    masks = [
        (lane >= own_rows) & (lane < own_rows + rim_rows // 2),
        lane < own_rows,
        (lane >= own_rows + rim_rows // 2) & (lane < rows),
    ]
    for u in range(owners):
        for x in range(cells_x):
            own = cells[u][x]
            turned_ref[x] = jnp.concatenate([own, own], axis=0).T
        for x in range(cells_x):
            image_ref[u, x * share : (x + 1) * share, :] = turned_ref[x, pl.ds(first, share), :]
    for pair, (u, v, oz) in enumerate(pairs_of(owners, places(me))):
        lhs = image_ref[u]
        products = [
            jnp.dot(lhs, weights_ref[3 * k + oz], preferred_element_type=jnp.float32) for k in range(3)
        ]
        for slot, x in enumerate([*range(cells_x), -1, cells_x]):
            total = None
            for k in range(3):
                source = x - (k - 1)
                if 0 <= source < cells_x:
                    term = products[k][source * share : (source + 1) * share, :]
                    total = term if total is None else total + term
            for oy, mask in enumerate(masks):
                tile = jnp.where(mask, total, 0.0).astype(jnp.bfloat16)
                out_ref[pair, slot, oy * share : (oy + 1) * share, :] = tile


def filled(pieces):
    pieces = list(pieces)
    missing = LANES - sum(p.shape[0] for p in pieces)
    return jnp.concatenate([*pieces, jnp.zeros((missing, pieces[0].shape[1]), pieces[0].dtype)], axis=0)


def putter(share, owners, out_ref, start=0):
    def put(n, u, value):
        out_ref[pl.ds((start * 27 + n) * owners + u, share, stride=27 * owners), :] = value

    return put


def sides(share, put, tiles_ref, pair, u, oz, face_ref, start, size):
    slot = tiles_ref.shape[1] - 2
    for side in range(2):
        left = jnp.concatenate(
            [tiles_ref[pair, slot + side, oy * share + start : oy * share + start + size, :] for oy in range(3)],
            axis=0,
        )
        value = jnp.dot(left, filled([face_ref[side]]), preferred_element_type=jnp.float32)
        for oy in range(3):
            put(18 * side + 3 * oy + oz, u, value[oy * size : (oy + 1) * size, :])


def middle_kernel(share, places, tiles_ref, *refs):
    owners = len(places(0))
    cells, rims, out_ref = refs[:owners], refs[owners : 2 * owners], refs[-1]
    cells_x = cells[0].shape[0]
    place = places(lax.axis_index("gz"))
    put = putter(share, owners, out_ref)
    zero = jnp.zeros((share, out_ref.shape[1]), jnp.float32)
    for u in range(owners):
        if owners == 2:
            lost = [1 - place[1 - u] + place[u]]
        else:
            lost = [oz for oz in range(3) if not 0 <= u + oz - 1 < owners]
        for oz in lost:
            for n in range(0, 27, 3):
                put(n + oz, place[u], zero)
    for pair, (u, v, oz) in enumerate(pairs_of(owners, place)):
        total = None
        for x in range(0, cells_x, 2):
            left = jnp.concatenate([tiles_ref[pair, x], tiles_ref[pair, x + 1]], axis=1)
            right = jnp.concatenate([filled([cells[v][i], rims[v][i]]) for i in (x, x + 1)], axis=0)
            term = jnp.dot(left, right, preferred_element_type=jnp.float32)
            total = term if total is None else total + term
        for oy in range(3):
            put(9 + 3 * oy + oz, place[u], total[oy * share : (oy + 1) * share, :])


def final_kernel(share, places, late, wide, tiles_ref, *refs):
    pieces, (_, whole_ref, out_ref, sem) = refs[:-4], refs[-4:]
    if len(pieces) == len(late):
        faces = dict(zip(late, pieces))
    else:
        beside, *across = pieces
        column = lax.axis_index("gx")
        odd = column % 2 == 1
        faces = {}
        for v in late:
            near, far = beside[v], across[v][...]
            zero = jnp.zeros_like(near)
            left, right = jnp.where(odd, near, far), jnp.where(odd, far, near)
            faces[v] = [jnp.where(column == 0, zero, left), jnp.where(column == wide - 1, zero, right)]
    owners = len(places(0))
    place = places(lax.axis_index("gz"))
    rounds = sem.shape[0]
    size = share // rounds
    copies = []
    for i in range(rounds):
        put = putter(size, owners, whole_ref, i * size)
        for pair, (u, v, oz) in enumerate(pairs_of(owners, place)):
            sides(share, put, tiles_ref, pair, place[u], oz, faces[v], i * size, size)
        span = pl.ds(i * size * 27 * owners, size * 27 * owners)
        copies.append(pltpu.make_async_copy(whole_ref.at[span], out_ref.at[span], sem.at[i]))
        copies[-1].start()
    for copy in copies:
        copy.wait()


def exchange(array, axes, flips, shift):
    sizes = [lax.axis_size(axis) for axis in axes]
    pairs = []
    for p in range(sizes[0]):
        to_p = (p + 1 if (p - shift) % 2 == 0 else p - 1) % sizes[0]
        if len(axes) == 1:
            pairs.append((p, to_p))
            continue
        for g in range(sizes[1]):
            pairs.append((p * sizes[1] + g, to_p * sizes[1] + (sizes[1] - 1 - g if flips else g)))
    return lax.ppermute(array, axes, pairs)


def sides_of(cells, rims):
    owners, cells_x = len(cells), cells[0].shape[0]
    wide, place = lax.axis_size("gx"), lax.axis_index("gx")

    def edge(v, x):
        return jnp.concatenate([cells[v][x], rims[v][x]], axis=0)

    if wide % 2 or owners != 2:
        left, right = halo(
            jnp.stack([edge(v, 0) for v in range(owners)]),
            jnp.stack([edge(v, cells_x - 1) for v in range(owners)]),
            "gx",
        )
    else:
        odd = place % 2 == 1
        across = jnp.where(odd, edge(0, cells_x - 1), edge(0, 0))
        far = exchange(across, ("gx", "gz"), True, 1)
        next_to = exchange(across, ("gx",), False, 1)
        beside = jnp.stack([jnp.where(odd, edge(v, 0), edge(v, cells_x - 1)) for v in range(owners)])
        beside = exchange(beside, ("gx",), False, 0)
        return [beside, next_to, far]
    return [jnp.stack([left[v], right[v]]) for v in range(owners)]


def in_hbm(array):
    return pltpu.with_memory_space_constraint(array, pltpu.HBM)


def cyclic(array, axis, step):
    peers = lax.axis_size(axis)
    return lax.ppermute(array, axis, [(i, (i + step) % peers) for i in range(peers)])


def halo(first, last, axis):
    peers, place = lax.axis_size(axis), lax.axis_index(axis)
    before = cyclic(last, axis, 1)
    after = cyclic(first, axis, -1)
    zero = jnp.zeros_like(before)
    return jnp.where(place == 0, zero, before), jnp.where(place == peers - 1, zero, after)


def columns(first, last):
    wide, peers = lax.axis_size("gx"), lax.axis_size("gy")
    if wide % 2:
        return halo(first, last, "gy")

    def target(p, q):
        if p % 2 == 0:
            return (p, q + 1) if q + 1 < peers else (p + 1, q)
        return (p, q - 1) if q > 0 else (p - 1, q)

    pairs = []
    for p in range(wide):
        for q in range(peers):
            to_p, to_q = target(p, q)
            pairs.append((p * peers + q, to_p * peers + to_q))
    place = lax.axis_index("gy")
    odd = lax.axis_index("gx") % 2 == 1
    ahead = lax.ppermute(jnp.where(odd, first, last), ("gx", "gy"), pairs)
    back = lax.ppermute(jnp.where(odd, last, first), ("gx", "gy"), [(t, f) for f, t in pairs])
    zero = jnp.zeros_like(ahead)
    before, after = jnp.where(odd, back, ahead), jnp.where(odd, ahead, back)
    return jnp.where(place == 0, zero, before), jnp.where(place == peers - 1, zero, after)


def line(array):
    owners = lax.axis_size("gz")
    if owners == 2:
        return [array, cyclic(array, "gz", 1)]
    gathered = lax.all_gather(array, "gz")
    return [gathered[v] for v in range(owners)]


def blocks(deflation, material, moduli, stencil):
    cells_x, cells_y, cells_z, parts, width = deflation.shape
    owners = lax.axis_size("gz")
    share = width // owners
    side = parts * cells_z
    own_rows = cells_y * side
    small = pltpu.CompilerParams(vmem_limit_bytes=16 << 20)
    vectors = jnp.transpose(deflation, (0, 1, 3, 2, 4))
    classes = jnp.transpose(material, (1, 2, 0))

    coupling = jnp.transpose(stencil, (1, 2, 0))
    scaled, coupling = pl.pallas_call(
        scale_kernel,
        out_shape=(
            jax.ShapeDtypeStruct((cells_x, own_rows, width), jnp.bfloat16),
            jax.ShapeDtypeStruct(coupling.shape, coupling.dtype),
        ),
        in_specs=[pl.BlockSpec(memory_space=pltpu.HBM)] * 4,
        out_specs=(pl.BlockSpec(memory_space=VMEM), pl.BlockSpec(memory_space=VMEM)),
        scratch_shapes=[
            pltpu.SMEM(moduli.shape, moduli.dtype),
            VMEM(classes.shape, classes.dtype),
            VMEM(vectors.shape, vectors.dtype),
            pltpu.SemaphoreType.DMA((3 + PIECES,)),
        ],
        compiler_params=small,
        name="scale",
    )(*(in_hbm(v) for v in (moduli, classes, vectors, coupling)))

    weights = pl.pallas_call(
        functools.partial(weight_kernel, cells_z),
        out_shape=jax.ShapeDtypeStruct((9, 2 * own_rows, LANES), jnp.bfloat16),
        in_specs=[pl.BlockSpec(memory_space=VMEM)],
        out_specs=pl.BlockSpec(memory_space=VMEM),
        compiler_params=small,
        name="weights",
    )(coupling)

    before, after = columns(scaled[:, :side], scaled[:, own_rows - side :])
    cells = line(scaled)
    rim = jnp.concatenate([before, after], axis=1)
    rims = line(rim)
    faces = sides_of(cells, rims)

    def places(me):
        return [me, 1 - me] if owners == 2 else list(range(owners))

    count = len(pairs_of(owners, places(0)))
    early = []
    late = [v for v in range(owners) if v not in early]
    in_vmem = pl.BlockSpec(memory_space=VMEM)
    tiles = pl.pallas_call(
        functools.partial(image_kernel, share, places, 2 * side),
        out_shape=jax.ShapeDtypeStruct((count, cells_x + 2, 3 * share, LANES), jnp.bfloat16),
        in_specs=[in_vmem] * (1 + owners),
        out_specs=in_vmem,
        scratch_shapes=[
            VMEM((cells_x, width, 2 * own_rows), jnp.bfloat16),
            VMEM((owners, cells_x * share, 2 * own_rows), jnp.bfloat16),
        ],
        compiler_params=small,
        name="image",
    )(weights, *cells)
    whole = jax.ShapeDtypeStruct((share * 27 * owners, width), jnp.float32)
    coarse = pl.pallas_call(
        functools.partial(middle_kernel, share, places),
        out_shape=pltpu.VMEM(whole.shape, whole.dtype),
        in_specs=[in_vmem] * (1 + 2 * owners + len(early)),
        out_specs=in_vmem,
        compiler_params=small,
        name="middle",
    )(tiles, *cells, *rims, *(faces[v] for v in early))
    _, coarse = pl.pallas_call(
        functools.partial(final_kernel, share, places, late, lax.axis_size("gx")),
        out_shape=(pltpu.VMEM(whole.shape, whole.dtype), whole),
        in_specs=[in_vmem] * (2 + len(faces)),
        out_specs=(in_vmem, pl.BlockSpec(memory_space=pltpu.HBM)),
        scratch_shapes=[pltpu.SemaphoreType.DMA((ROUNDS,))],
        input_output_aliases={1 + len(faces): 0},
        compiler_params=small,
        name="final",
    )(tiles, *faces, coarse)
    coarse = coarse.reshape(share, 27, owners, width)
    return jnp.transpose(coarse, (0, 2, 1, 3)).reshape(1, 1, share, owners, 27, width)


def solution(mesh):
    in_specs = (P("gx", "gy", "gz", None, None), P("gx", "gy", "gz"), P(), P())
    out_specs = P("gx", "gy", "gz", None, None, None)
    return jax.shard_map(blocks, mesh=mesh, in_specs=in_specs, out_specs=out_specs, check_vma=False)
```
